32 devices in a mesh: gx: 8 (over z, core), gy: 4 (over y, x).
Axes of the slice: x: 2, y: 2, z: 4, core: 2. Of those that a mesh axis runs over, the one named last changes fastest.
Arguments:
- velocity: float32 [3, 128, 64, 128], P(None, 'gx', 'gy'), may hold values from -6 to 6
- stresses: float32 [6, 128, 64, 128], P(None, 'gx', 'gy'), may hold values from -6 to 6
- buoyancy: float32 [128, 64, 128], P('gx', 'gy'), may hold values from 0.3 to 0.6
- lame_first: float32 [128, 64, 128], P('gx', 'gy'), may hold values from 0.05 to 0.15
- rigidity: float32 [128, 64, 128], P('gx', 'gy'), may hold values from 0.04 to 0.12
- histories: bfloat16 [8192, 512], P(('gx', 'gy')), may hold values from -6 to 6
- mechanism: bfloat16 [8192, 6], P(('gx', 'gy')), may hold values from -6 to 6
- resample: bfloat16 [512, 3], replicated, may hold values from -0.25 to 0.25
- owners: int32 [8192, 1], P(('gx', 'gy')), may hold values from 0 to 3; in each aligned block of 256 rows (0 to 255, 256 to 511, ...) at most 64 rows name the same one
- cell_offsets: int32 [8192], P(('gx', 'gy')), may hold values from 0 to 32767
Outputs:
- velocity_out: float32 [3, 128, 64, 128], P(None, 'gx', 'gy')
- stresses_out: float32 [6, 128, 64, 128], P(None, 'gx', 'gy')
The draws below stay inside these ranges and needn't reach their ends.
Inputs may be any that keep to these rules, and one draw needn't show every extreme that they name: `owners`: among the 256 rows of one device at most 64 name the same owner, a bound that some block reaches of them. `cell_offsets`: cell index x * 16 * 128 + y * 128 + z within the enclosing block.
All inputs are finite; a program needn't handle non-finite values.
Results may differ from the reference program's by a relative error of at most 0.00052.
Values may be sent and summed in bfloat16 or wider, within the bound.
A program may use at most 64 MiB of HBM per device.

```python
import math
import jax
import jax.numpy as jnp
import numpy as np
from jax import lax

CX = 16
CY = 16
CZ = 128
STEPS = 3
SAMPLES = 512
SRC_DEV = 256
CAP = 64
NX = 128
NY = 64
SOURCES = 8192
N_GY = 4


def plant(values, stream_key, least, high):
    shape = values.shape
    place = [jax.random.randint(jax.random.fold_in(stream_key, axis), (), 0, shape[axis]) for axis in range(len(shape))]
    values = values.at[tuple(place)].set(least)
    longest = shape.index(max(shape))
    place[longest] = (place[longest] + 1) % shape[longest]
    return values.at[tuple(place)].set(high)


def block_levels(rng, dims, shards, least, high):
    def one(position, blocks):
        heights = jax.random.uniform(jax.random.fold_in(jax.random.fold_in(rng, 6), position), (blocks,), jnp.float32, least / len(shards), high / len(shards))
        return jnp.repeat(jnp.exp(heights), dims[position] // blocks).reshape((-1,) + (1,) * (len(dims) - position - 1))

    gain = one(*shards[0])
    for cut in shards[1:]:
        gain = gain * one(*cut)
    return gain


def routed_block(key, own, number, rows, count, top, bound, skew):
    sequence = jax.random.permutation(key, count)
    packed, ordinary = shares(count, rows * top, bound, skew, True), shares(count, rows * top, bound, skew, False)
    places = jnp.arange(count)

    def named(lengths, turn):
        used = int((lengths > 0).sum())
        fixed = max(1, used // 4)
        moved = fixed + (places - fixed + turn * (used - fixed)) % max(1, count - fixed)
        return jnp.zeros((count,), jnp.int32).at[sequence[jnp.where(places < fixed, places, moved)]].set(jnp.asarray(lengths, jnp.int32))

    lengths = jnp.where(number % 4 == 0, named(packed, number // 4), named(ordinary, number - number // 4 - 1))
    mixed = jax.random.permutation(jax.random.fold_in(own, 3), count)
    donor, taker = mixed[0:count // 2 * 2:2], mixed[1:count // 2 * 2:2]
    margin = jnp.minimum(lengths[donor] - 1, bound - lengths[taker]) // 2
    margin = jnp.where((donor == sequence[0]) | (taker == sequence[0]) | (lengths[taker] == 0), 0, jnp.maximum(margin, 0))
    moved = jax.random.randint(jax.random.fold_in(own, 4), (count // 2,), 0, 1 << 20) % (margin + 1)
    lengths = lengths.at[donor].add(-moved).at[taker].add(moved)
    items = jnp.searchsorted(jnp.cumsum(lengths), jnp.arange(rows * top), side="right").astype(jnp.int32)
    table = items.reshape(top, rows).T
    table = table[jax.random.permutation(jax.random.fold_in(own, 1), rows)]
    turn = jax.random.randint(jax.random.fold_in(own, 2), (rows, 1), 0, top)
    return jnp.take_along_axis(table, (jnp.arange(top)[None, :] + turn) % top, axis=1)


def shares(number_of, total, bound, skew, full):
    portions = [(1 << 20) // math.isqrt(standing ** skew) + 1 for standing in range(1, number_of + 1)]
    largest = bound if full else min(bound, max(-(-total // number_of), total * portions[0] // sum(portions)))
    least = 1 if total - largest >= number_of - 1 else 0
    counts, spare = [largest] + [least] * (number_of - 1), total - largest - least * (number_of - 1)
    while spare > 0:
        movable = [i for i in range(1, number_of) if counts[i] < largest] or [i for i in range(1, number_of) if counts[i] < bound]
        whole, left = sum([portions[i] for i in movable]), spare
        for i in movable:
            extra = min(bound - counts[i], max(1, left * portions[i] // whole), spare)
            counts[i] = counts[i] + extra
            spare = spare - extra
    return np.array(counts)


def noise(stream_key, dims, width, limit, split=(), kind=jnp.bfloat16):
    drawn = jax.random.normal(stream_key, dims, jnp.float32) * width
    if len(split) > 0:
        drawn = block_levels(stream_key, dims, split, -0.22, 0.18) * drawn
    return jnp.clip(drawn, min=-limit, max=limit).astype(kind)


def setup_inputs(seed: int = 0) -> dict:
    arg_keys = jax.random.split(jax.random.key(seed), 11)
    velocity = noise(arg_keys[0], (3, NX, NY, CZ), 1.0, 6.0, ((1, 8), (2, 4)), jnp.float32)
    stresses = noise(arg_keys[1], (6, NX, NY, CZ), 1.0, 6.0, ((1, 8), (2, 4)), jnp.float32)
    buoyancy = jnp.clip(jnp.exp(math.log(0.6) - 0.6931472 * jax.random.uniform(arg_keys[2], (NX, NY, CZ), jnp.float32) ** block_levels(arg_keys[2], (NX, NY, CZ), ((0, 8), (1, 4)), -0.2, 0.2)), 0.3, 0.6)
    lame_first = jnp.clip(0.05 + 0.10000001 * jax.random.uniform(arg_keys[3], (NX, NY, CZ), jnp.float32) ** block_levels(arg_keys[3], (NX, NY, CZ), ((0, 8), (1, 4)), -0.2, 0.2), 0.05, 0.15)
    rigidity = jnp.clip(jnp.exp(math.log(0.12) - 1.0986123 * jax.random.uniform(arg_keys[4], (NX, NY, CZ), jnp.float32) ** block_levels(arg_keys[4], (NX, NY, CZ), ((0, 8), (1, 4)), -0.2, 0.2)), 0.04, 0.12)
    histories = noise(arg_keys[5], (SOURCES, SAMPLES), 1.0, 6.0, ((0, 32),))
    mechanism = noise(arg_keys[6], (SOURCES, 6), 1.0, 6.0, ((0, 32),))
    resample = noise(arg_keys[7], (SAMPLES, STEPS), SAMPLES ** -0.5, 0.25)
    owners_keys = jax.random.split(jax.random.fold_in(arg_keys[8], 1), SOURCES // SRC_DEV)
    owners_turns = jax.random.permutation(jax.random.fold_in(arg_keys[8], 3), SOURCES // SRC_DEV)
    owners = jax.vmap(lambda own, number: routed_block(jax.random.fold_in(arg_keys[8], 2), own, number, SRC_DEV, N_GY, 1, CAP, 2))(owners_keys, owners_turns).reshape((SOURCES, 1))
    cell_offsets = plant(jax.random.randint(arg_keys[9], (SOURCES,), 0, CX * CY * CZ), jax.random.fold_in(arg_keys[9], 1), 0, (CX * CY * CZ) - 1).astype(jnp.int32)
    return {"velocity": velocity, "stresses": stresses, "buoyancy": buoyancy, "lame_first": lame_first, "rigidity": rigidity, "histories": histories, "mechanism": mechanism, "resample": resample, "owners": owners, "cell_offsets": cell_offsets}


INNER_WEIGHT = 9.0 / 8.0
OUTER_WEIGHT = -1.0 / 24.0


def differ(values, dimension, forward):
    if dimension == 2:
        values = jnp.pad(values, ((0, 0), (0, 0), (2, 2)))
    extent = values.shape[dimension] - 4

    def window(start_at):
        return lax.slice_in_dim(values, start_at, start_at + extent, axis=dimension)

    if forward:
        result = INNER_WEIGHT * (window(3) - window(2)) + OUTER_WEIGHT * (window(4) - window(1))
    else:
        result = INNER_WEIGHT * (window(2) - window(1)) + OUTER_WEIGHT * (window(3) - window(0))
    for second in (0, 1):
        if second != dimension:
            result = lax.slice_in_dim(result, 2, result.shape[second] - 2, axis=second)
    return result


def advance_velocity(velocity, stresses, buoyancy):
    forces = jnp.stack([
        differ(stresses[0], 0, True) + differ(stresses[3], 1, False) + differ(stresses[4], 2, False),
        differ(stresses[3], 0, False) + differ(stresses[1], 1, True) + differ(stresses[5], 2, False),
        differ(stresses[4], 0, False) + differ(stresses[5], 1, False) + differ(stresses[2], 2, True),
    ])
    return velocity + buoyancy * forces


def advance_stress(stresses, velocity, lame_first, rigidity):
    stretch_one = differ(velocity[0], 0, False)
    stretch_two = differ(velocity[1], 1, False)
    stretch_three = differ(velocity[2], 2, False)
    change = stretch_one + stretch_two + stretch_three
    rates = jnp.stack([
        lame_first * change + 2.0 * rigidity * stretch_one,
        lame_first * change + 2.0 * rigidity * stretch_two,
        lame_first * change + 2.0 * rigidity * stretch_three,
        rigidity * (differ(velocity[0], 1, True) + differ(velocity[1], 0, True)),
        rigidity * (differ(velocity[0], 2, True) + differ(velocity[2], 0, True)),
        rigidity * (differ(velocity[1], 2, True) + differ(velocity[2], 1, True)),
    ])
    return stresses + rates


def reference(velocity, stresses, buoyancy, lame_first, rigidity, histories, mechanism, resample, owners, cell_offsets):
    amplitude = jnp.dot(histories, resample, preferred_element_type=jnp.float32)
    terms = (mechanism.astype(jnp.float32)[:, :, None] * amplitude[:, None, :]).astype(jnp.bfloat16)
    device = jnp.arange(SOURCES, dtype=jnp.int32) // SRC_DEV
    across_cells = (device // N_GY) * CX + cell_offsets // (CY * CZ)
    normal_cells = owners[:, 0] * CY + (cell_offsets // CZ) % CY
    depth_cells = cell_offsets % CZ
    border = ((0, 0), (2, 2), (2, 2), (0, 0))
    for step_index in range(STEPS):
        velocity = advance_velocity(velocity, jnp.pad(stresses, border), buoyancy)
        stresses = advance_stress(stresses, jnp.pad(velocity, border), lame_first, rigidity)
        stresses = stresses.at[:, across_cells, normal_cells, depth_cells].add(terms[:, :, step_index].astype(jnp.float32).T)
    return velocity, stresses
```

```python
import functools

import jax
import jax.numpy as jnp
from jax import lax
from jax.experimental import pallas as pl
from jax.experimental.pallas import tpu as pltpu
from jax.sharding import PartitionSpec as P

A = 9.0 / 8.0
B = -1.0 / 24.0
MESH = pl.DeviceIdType.MESH
XP = 2
YP = 8

STRESS_FACES = (((0, True), (3, False), (4, False)), ((3, False), (1, True), (5, False)))
VELOCITY_FACES = (((0, False), (1, True), (2, True)), ((0, True), (1, False), (2, True)))


def face_layers(faces, up, extent):
    edge, inward = (extent - 1, -1) if up else (0, 1)
    out, at = [], 0
    for comp, forward in faces:
        wide = forward != up
        out.append((comp, 0, edge, wide, at))
        at += 2 if wide else 1
        if wide:
            out.append((comp, 1, edge + inward, False, at))
            at += 1
    return out


def face_slots(faces, up, extent):
    return sum(2 if wide else 1 for _, _, _, wide, _ in face_layers(faces, up, extent))


def unpacker(faces, up, extent, slot):
    places = {(comp, order): (at, wide) for comp, order, _, wide, at in face_layers(faces, up, extent)}

    def halo(comp, order):
        at, wide = places[comp, order]
        value = slot(at).astype(jnp.float32)
        return value + slot(at + 1).astype(jnp.float32) if wide else value

    return halo


def halo_terms(faces, from_low, extent, halo):
    edge, inward = (0, 1) if from_low else (extent - 1, -1)
    sign = -1.0 if from_low else 1.0
    out = []
    for comp, forward in faces:
        if from_low == forward:
            out.append((comp, 0, edge, sign * B * halo(comp, 0)))
            continue
        first, second = halo(comp, 0), halo(comp, 1)
        out.append((comp, 0, edge, sign * A * first + sign * B * second))
        out.append((comp, 1, edge + inward, sign * B * first))
    return out


def kernel(
    groups, blocks, steps,
    v_hbm, s_hbm, buoy_hbm, lame_hbm, rig_hbm, hist_hbm, mech_hbm, res_hbm, own_hbm, off_hbm,
    v_out, s_out,
    V, S, buoy, lame, rig, hist, mech_ref, res_ref, own_ref, off_ref, src, gathered, plane_hot, level_hot,
    send_x, recv_x, send_y, recv_y, corner_out, corner_in, edge_x, edge_y_out, edge_y, own_x, own_y,
    stress_sem, load_sem, src_send, src_recv, face_send, face_recv,
    corner_send, corner_recv, edge_send, edge_recv,
):
    gx = lax.axis_index("gx")
    gy = lax.axis_index("gy")
    cx, cy, cz = buoy.shape
    rows = hist.shape[0]
    inner = (slice(None), pl.ds(XP, cx), pl.ds(YP, cy), slice(None))

    barrier = pltpu.get_barrier_semaphore()
    sides = (
        (gx > 0, (gx - 1, gy)),
        (gx < blocks - 1, (gx + 1, gy)),
        (gy > 0, (gx, gy - 1)),
        (gy < groups - 1, (gx, gy + 1)),
    )
    for there, device in sides[:2]:
        @pl.when(there)
        def _(device=device):
            pl.semaphore_signal(barrier, inc=1, device_id=device, device_id_type=MESH)
    corners = []
    for ux in range(2):
        for uy in range(2):
            there = jnp.logical_and(sides[ux][0], sides[2 + uy][0])
            corners.append((there, (gx + 2 * ux - 1, gy + 2 * uy - 1)))
    for there, device in corners:
        @pl.when(there)
        def _(device=device):
            pl.semaphore_signal(barrier, inc=1, device_id=device, device_id_type=MESH)
    for k in range(1, groups):
        pl.semaphore_signal(
            barrier, inc=1, device_id=(gx, lax.rem(gy + k, groups)), device_id_type=MESH
        )

    loads = [
        pltpu.make_async_copy(hist_hbm, hist, load_sem.at[0]),
        pltpu.make_async_copy(v_hbm, V.at[inner], load_sem.at[1]),
        pltpu.make_async_copy(buoy_hbm, buoy, load_sem.at[2]),
        pltpu.make_async_copy(lame_hbm, lame, load_sem.at[3]),
        pltpu.make_async_copy(rig_hbm, rig, load_sem.at[4]),
        pltpu.make_async_copy(mech_hbm, mech_ref, load_sem.at[5]),
        pltpu.make_async_copy(res_hbm, res_ref, load_sem.at[6]),
        pltpu.make_async_copy(own_hbm, own_ref, load_sem.at[7]),
        pltpu.make_async_copy(off_hbm, off_ref, load_sem.at[8]),
    ]
    stress_loads = {
        comp: pltpu.make_async_copy(
            s_hbm.at[comp], S.at[(comp,) + inner[1:]], stress_sem.at[comp]
        )
        for comp in (3, 1, 5, 0, 4, 2)
    }
    for load in list(stress_loads.values()) + loads:
        load.start()

    for ref in (V, S):
        zero_x = jnp.zeros((ref.shape[0], XP, cy, cz), jnp.float32)
        ref[:, pl.ds(0, XP), pl.ds(YP, cy), :] = zero_x
        ref[:, pl.ds(XP + cx, XP), pl.ds(YP, cy), :] = zero_x

        def clear(x, carry, ref=ref):
            zero_y = jnp.zeros((ref.shape[0], YP, cz), jnp.float32)
            ref[:, XP + x, pl.ds(0, YP), :] = zero_y
            ref[:, XP + x, pl.ds(YP + cy, YP), :] = zero_y
            return carry

        lax.fori_loop(0, cx, clear, 0)

    def face_copy(phase, side, faces):
        axis, up = side // 2, side % 2
        send, recv = ((send_x, recv_x), (send_y, recv_y))[axis]
        count = face_slots(faces[axis], bool(up), (cx, cy)[axis])
        return pltpu.make_async_remote_copy(
            src_ref=send.at[phase, up, pl.ds(0, count)],
            dst_ref=recv.at[phase, up, pl.ds(0, count)],
            send_sem=face_send.at[phase, side],
            recv_sem=face_recv.at[phase, side],
            device_id=sides[side][1],
            device_id_type=MESH,
        )

    def row(ref, comp, axis, layer):
        x, y = (XP, YP) if ref is V or ref is S else (0, 0)
        if axis == 0:
            return ref.at[comp, x + layer, pl.ds(y, cy), :]
        return ref.at[comp, pl.ds(x, cx), y + layer, :]

    def coefficient(ref, axis, layer):
        return ref[layer] if axis == 0 else ref[:, layer, :]

    odd = lax.rem(gy, 2) == 1
    even = jnp.logical_not(odd)
    near = ((2, jnp.logical_and(sides[2][0], odd)), (3, jnp.logical_and(sides[3][0], even)))
    far = ((3, jnp.logical_and(sides[3][0], odd)), (2, jnp.logical_and(sides[2][0], even)))
    across = ((0, sides[0][0]), (1, sides[1][0]))

    def send_face(side, phase, ref, faces):
        axis, up = side // 2, side % 2
        send = (send_x, send_y)[axis]
        for comp, _, layer, wide, at in face_layers(faces[axis], bool(up), (cx, cy)[axis]):
            value = row(ref, comp, axis, layer)[...]
            head = value.astype(jnp.bfloat16)
            send[phase, up, at] = head
            if wide:
                rest = value - head.astype(jnp.float32)
                send[phase, up, at + 1] = rest.astype(jnp.bfloat16)
        face_copy(phase, side, faces).start()

    def receive_face(side, phase, faces, apply, partial=None):
        axis, up = side // 2, side % 2
        extent = (cx, cy)[axis]
        recv = (recv_x, recv_y)[axis]
        face_copy(phase, 2 * axis + 1 - up, faces).wait_recv()
        arrived = unpacker(faces[axis], not up, extent, lambda at: recv[phase, 1 - up, at])
        halo = arrived if partial is None else lambda comp, order: arrived(comp, order) + partial(side, comp, order)
        for comp, _, layer, value in halo_terms(faces[axis], not up, extent, halo):
            apply(axis, comp, layer, value)

    def edge_copy(side):
        axis, up = side // 2, side % 2
        if axis == 0:
            src, dst = buoy.at[pl.ds(cx - 2 if up else 0, 2)], edge_x.at[up]
        else:
            src, dst = edge_y_out.at[up], edge_y.at[up]
        return pltpu.make_async_remote_copy(
            src_ref=src, dst_ref=dst,
            send_sem=edge_send.at[side], recv_sem=edge_recv.at[side],
            device_id=sides[side][1], device_id_type=MESH,
        )

    def send_edge(side):
        axis, up = side // 2, side % 2
        if axis == 1:
            for order in range(2):
                edge_y_out[up, order] = buoy[:, cy - 1 - order if up else order, :]
        edge_copy(side).start()

    def edge_index(axis, up, order):
        return 1 - order if axis == 0 and up else order

    velocity_places = [
        [
            {(comp, order): k for k, (comp, order, *_) in enumerate(face_layers(VELOCITY_FACES[axis], not up, extent))}
            for up in (False, True)
        ]
        for axis, extent in enumerate((cx, cy))
    ]
    force_of = ({0: 0, 3: 1, 4: 2}, {3: 0, 1: 1, 5: 2})
    owns, edges = (own_x, own_y), (edge_x, edge_y)

    def own_part(side, phase):
        axis, up = side // 2, side % 2
        send = (send_x, send_y)[axis]
        halo = unpacker(STRESS_FACES[axis], bool(up), (cx, cy)[axis], lambda at: send[phase, up, at])
        for comp, order, _, value in halo_terms(STRESS_FACES[axis], bool(up), (cx, cy)[axis], halo):
            k = velocity_places[axis][up][force_of[axis][comp], order]
            factor = edges[axis][1 - up, edge_index(axis, 1 - up, order)]
            owns[axis][up, k] = factor * value

    def partial_velocity(side, comp, order):
        axis, up = side // 2, side % 2
        return owns[axis][up, velocity_places[axis][up][comp, order]]

    corner_comps = (0, 1, 3, 4, 5)

    def corner_copy(t, corner):
        return pltpu.make_async_remote_copy(
            src_ref=corner_out.at[t, corner], dst_ref=corner_in.at[t, corner],
            send_sem=corner_send.at[t, corner], recv_sem=corner_recv.at[t, corner],
            device_id=corners[corner][1], device_id_type=MESH,
        )

    def send_corner(t, corner):
        ux, uy = corner // 2, corner % 2
        for i, comp in enumerate(corner_comps):
            for xi in range(2):
                x, y = (cx - 2 if ux else 0) + xi, cy - 2 if uy else 0
                corner_out[t, corner, pl.ds(4 * i + 2 * xi, 2), :] = S[comp, XP + x, pl.ds(YP + y, 2), :]
        corner_copy(t, corner).start()

    def receive_corner(t, corner):
        ups = (corner // 2, corner % 2)
        corner_copy(t, 3 - corner).wait_recv()

        def stress(comp, orders):
            xi, yi = (order if up else 1 - order for up, order in zip(ups, orders))
            return corner_in[t, 3 - corner, pl.ds(4 * corner_comps.index(comp) + 2 * xi + yi, 1), :]

        for axis in range(2):
            up, other = ups[axis], 1 - axis
            extent = (cx, cy)[other]
            for (vcomp, order), k in velocity_places[axis][up].items():
                edge = edge_index(axis, 1 - up, order)

                def halo(comp, across):
                    return stress(comp, (order, across) if axis == 0 else (across, order))

                faces = [f for f in STRESS_FACES[other] if force_of[other][f[0]] == vcomp]
                for _, _, layer, value in halo_terms(faces, not ups[other], extent, halo):
                    place = owns[axis].at[up, k, pl.ds(layer, 1), :]
                    place[...] = place[...] + edges[axis][1 - up, edge, pl.ds(layer, 1), :] * value

    def at_corners(*actions):
        for corner, (there, _) in enumerate(corners):
            @pl.when(there)
            def _(corner=corner):
                for action in actions:
                    action(corner)

    def at_sides(which, *actions):
        for side, there in which:
            @pl.when(there)
            def _(side=side):
                for action in actions:
                    action(side)

    def finish_faces(phase, faces):
        for side in (0, 1, 2, 3):
            @pl.when(sides[side][0])
            def _(side=side):
                face_copy(phase, side, faces).wait_send()

    def add(ref, comp, axis, layer, value):
        place = row(ref, comp, axis, layer)
        place[...] = place[...] + value

    def apply_force(axis, comp, layer, value):
        add(V, force_of[axis][comp], axis, layer, coefficient(buoy, axis, layer) * value)

    shear_of = ({1: 3, 2: 4}, {0: 3, 2: 5})

    def apply_strain(target, axis, comp, layer, value):
        mu = coefficient(rig, axis, layer)
        if comp != axis:
            add(target, shear_of[axis][comp], axis, layer, mu * value)
            return
        volume = coefficient(lame, axis, layer) * value
        for normal in range(3):
            extra = volume + 2.0 * mu * value if normal == axis else volume
            add(target, normal, axis, layer, extra)

    level = lax.broadcasted_iota(jnp.int32, (cy, cz), 1)

    def along_z(values, by):
        moved = pltpu.roll(values, (-by) % cz, 1)
        return jnp.where(level < cz - by if by > 0 else level >= -by, moved, 0.0)

    def differ(ref, comp, x, dimension, forward):
        def window(by):
            if dimension == 0:
                return ref[comp, XP + x + by, pl.ds(YP, cy), :]
            if dimension == 1:
                return ref[comp, XP + x, pl.ds(YP + by, cy), :]
            values = ref[comp, XP + x, pl.ds(YP, cy), :]
            return along_z(values, by) if by else values

        if forward:
            return A * (window(1) - window(0)) + B * (window(2) - window(-1))
        return A * (window(0) - window(-1)) + B * (window(1) - window(-2))

    def velocity_inner(x, carry):
        force = (
            differ(S, 0, x, 0, True) + differ(S, 3, x, 1, False) + differ(S, 4, x, 2, False),
            differ(S, 3, x, 0, False) + differ(S, 1, x, 1, True) + differ(S, 5, x, 2, False),
            differ(S, 4, x, 0, False) + differ(S, 5, x, 1, False) + differ(S, 2, x, 2, True),
        )
        factor = buoy[x]
        for comp in range(3):
            place = V.at[comp, XP + x, pl.ds(YP, cy), :]
            place[...] = place[...] + factor * force[comp]
        return carry

    def stress_inner(last, x, carry):
        one = differ(V, 0, x, 0, False)
        two = differ(V, 1, x, 1, False)
        three = differ(V, 2, x, 2, False)
        mu = rig[x]
        volume = lame[x] * (one + two + three)
        rates = (
            volume + 2.0 * mu * one,
            volume + 2.0 * mu * two,
            volume + 2.0 * mu * three,
            mu * (differ(V, 0, x, 1, True) + differ(V, 1, x, 0, True)),
            mu * (differ(V, 0, x, 2, True) + differ(V, 2, x, 0, True)),
            mu * (differ(V, 1, x, 2, True) + differ(V, 2, x, 1, True)),
        )
        for comp in range(6):
            place = S.at[comp, XP + x, pl.ds(YP, cy), :]
            target = s_out.at[comp, x] if last else place
            target[...] = place[...] + rates[comp]
        if last:
            for comp in range(3):
                v_out[comp, x] = V[comp, XP + x, pl.ds(YP, cy), :]
        return carry

    def sweep(body):
        batch = 2 if cx % 2 == 0 else 1

        def several(at, carry):
            for one in range(batch):
                carry = body(batch * at + one, carry)
            return carry

        lax.fori_loop(0, cx // batch, several, 0)

    def source_copy(k):
        return pltpu.make_async_remote_copy(
            src_ref=src,
            dst_ref=gathered.at[:, pl.ds(k * rows, rows)],
            send_sem=src_send.at[k],
            recv_sem=src_recv.at[k],
            device_id=(gx, lax.rem(gy + k, groups)),
            device_id_type=MESH,
        )

    comps = src.shape[0] // (steps + 1)

    def source_terms():
        contract_last = (((1,), (1,)), ((), ()))
        amplitude = lax.dot_general(
            res_ref[...], hist[...], contract_last, preferred_element_type=jnp.float32
        )
        mech = mech_ref[...].astype(jnp.float32)
        spare = jnp.zeros((comps - mech.shape[0], rows), jnp.float32)
        parts = []
        for t in range(steps):
            parts += [mech * amplitude[t : t + 1, :], spare]
        offsets = off_ref[...]
        places = [own_ref[...], offsets // (cy * cz), (offsets // cz) % cy, offsets % cz]
        places = [p.astype(jnp.float32) for p in places]
        parts += [jnp.concatenate(places + [jnp.zeros((comps - 4, rows), jnp.float32)], axis=0)]
        packed = jnp.concatenate(parts, axis=0).astype(jnp.bfloat16)
        src[...] = packed
        gathered[:, pl.ds(0, rows)] = packed

    def source_masks():
        for k in range(groups):
            lanes = pl.ds(k * rows, rows)
            info = gathered[pl.ds(steps * comps, comps), lanes].astype(jnp.float32)
            cell_plane = info[0:1] * float(cx * cy) + info[1:2] * float(cy) + info[2:3]
            plane = lax.broadcasted_iota(jnp.int32, (cx * cy, rows), 0) + gy * (cx * cy)
            plane_hot[:, lanes] = jnp.where(
                plane == cell_plane.astype(jnp.int32), 1.0, 0.0
            ).astype(jnp.bfloat16)
            height = lax.broadcasted_iota(jnp.int32, (cz, rows), 0)
            level_hot[:, lanes] = jnp.where(
                height == info[3:4].astype(jnp.int32), 1.0, 0.0
            ).astype(jnp.bfloat16)

    def insert_sources(t):
        values = gathered[pl.ds(t * comps, comps), :].astype(jnp.float32)
        for comp in range(0, 6, 2):
            spread = jnp.concatenate(
                [
                    level_hot[...] * values[c : c + 1, :].astype(jnp.bfloat16)
                    for c in (comp, comp + 1)
                ],
                axis=0,
            )
            placed = lax.dot_general(
                plane_hot[...], spread, (((1,), (1,)), ((), ())),
                preferred_element_type=jnp.float32,
            )
            for c in range(2):
                place = S.at[comp + c, pl.ds(XP, cx), pl.ds(YP, cy), :]
                place[...] = place[...] + placed[:, c * cz : (c + 1) * cz].reshape(cx, cy, cz)

    arrivals = groups - 1
    for there, _ in list(sides[:2]) + corners:
        arrivals += there.astype(jnp.int32)

    def send_stress(t):
        def send(side):
            send_face(side, 2 * t, S, STRESS_FACES)

        at_sides(far, send)
        at_corners(functools.partial(send_corner, t))
        at_sides(near, send)
        at_sides(across, send)

    for load in [loads[0]] + loads[5:]:
        load.wait()
    source_terms()
    pl.semaphore_wait(barrier, arrivals)
    for load in stress_loads.values():
        load.wait()
    send_stress(0)
    for k in range(1, groups):
        source_copy(k).start()
    loads[1].wait()
    loads[2].wait()
    everywhere = far + near + across
    at_sides(everywhere, send_edge)
    for t in range(steps):
        first, second = 2 * t, 2 * t + 1
        last = t == steps - 1
        sweep(velocity_inner)
        at_sides(everywhere, lambda side: send_face(side, second, V, VELOCITY_FACES))
        if t > 0:
            at_sides(everywhere, lambda side: own_part(side, first))
            insert_sources(t)
        at_sides(across + near + far, lambda side: receive_face(side, first, STRESS_FACES, apply_force))
        if t == 0:
            loads[3].wait()
            loads[4].wait()
            at_sides(across + near + far, lambda side: edge_copy(2 * (side // 2) + 1 - side % 2).wait_recv())
            at_sides(everywhere, lambda side: own_part(side, first))
            if last:
                for k in range(1, groups):
                    source_copy(k).wait_recv()
                source_masks()
                insert_sources(0)
        sweep(functools.partial(stress_inner, last))
        if t == 0 and not last:
            for k in range(1, groups):
                source_copy(k).wait_recv()
            source_masks()
            insert_sources(0)
        at_corners(functools.partial(receive_corner, t))
        strain = functools.partial(apply_strain, s_out if last else S)
        at_sides(
            across + near + far,
            lambda side: receive_face(side, second, VELOCITY_FACES, strain, partial_velocity),
        )
        if not last:
            send_stress(t + 1)
    for t in range(steps):
        finish_faces(2 * t, STRESS_FACES)
        finish_faces(2 * t + 1, VELOCITY_FACES)
        at_corners(lambda corner: corner_copy(t, corner).wait_send())
    at_sides(everywhere, lambda side: edge_copy(side).wait_send())
    for k in range(1, groups):
        source_copy(k).wait_send()


def store_kernel(v_ref, s_ref, v_out, s_out, sem):
    copies = [pltpu.make_async_copy(v_ref, v_out, sem.at[0])]
    half = s_ref.shape[0] // 2
    for part in range(2):
        layers = pl.ds(part * half, half)
        copies.append(pltpu.make_async_copy(s_ref.at[layers], s_out.at[layers], sem.at[1 + part]))
    for copy in copies:
        copy.start()
    for copy in copies:
        copy.wait()


def local(
    velocity, stresses, buoyancy, lame_first, rigidity,
    histories, mechanism, resample, owners, cell_offsets,
):
    groups = lax.axis_size("gy")
    blocks = lax.axis_size("gx")
    rows, samples = histories.shape
    steps = resample.shape[1]
    _, cx, cy, cz = velocity.shape
    comps = 8
    tall = comps * (steps + 1)
    f32, bf16 = jnp.float32, jnp.bfloat16
    hbm = pl.BlockSpec(memory_space=pl.ANY)
    vmem = pl.BlockSpec(memory_space=pltpu.VMEM)
    dma = pltpu.SemaphoreType.DMA
    phases = 2 * steps
    v_last, s_last = pl.pallas_call(
        functools.partial(kernel, groups, blocks, steps),
        out_shape=(
            pltpu.VMEM(velocity.shape, f32),
            pltpu.VMEM(stresses.shape, f32),
        ),
        in_specs=[hbm] * 10,
        out_specs=(vmem, vmem),
        scratch_shapes=[
            pltpu.VMEM((3, cx + 2 * XP, cy + 2 * YP, cz), f32),
            pltpu.VMEM((6, cx + 2 * XP, cy + 2 * YP, cz), f32),
            pltpu.VMEM((cx, cy, cz), f32),
            pltpu.VMEM((cx, cy, cz), f32),
            pltpu.VMEM((cx, cy, cz), f32),
            pltpu.VMEM((rows, samples), bf16),
            pltpu.VMEM((mechanism.shape[1], rows), bf16),
            pltpu.VMEM((steps, samples), bf16),
            pltpu.VMEM((1, rows), jnp.int32),
            pltpu.VMEM((1, rows), jnp.int32),
            pltpu.VMEM((tall, rows), bf16),
            pltpu.VMEM((tall, groups * rows), bf16),
            pltpu.VMEM((cx * cy, groups * rows), bf16),
            pltpu.VMEM((cz, groups * rows), bf16),
            pltpu.VMEM((phases, 2, 9, cy, cz), bf16),
            pltpu.VMEM((phases, 2, 9, cy, cz), bf16),
            pltpu.VMEM((phases, 2, 9, cx, cz), bf16),
            pltpu.VMEM((phases, 2, 9, cx, cz), bf16),
            pltpu.VMEM((steps, 4, 24, cz), f32),
            pltpu.VMEM((steps, 4, 24, cz), f32),
            pltpu.VMEM((2, 2, cy, cz), f32),
            pltpu.VMEM((2, 2, cx, cz), f32),
            pltpu.VMEM((2, 2, cx, cz), f32),
            pltpu.VMEM((2, 5, cy, cz), f32),
            pltpu.VMEM((2, 5, cx, cz), f32),
            dma((6,)),
            dma((9,)),
            dma((groups,)),
            dma((groups,)),
            dma((phases, 4)),
            dma((phases, 4)),
            dma((steps, 4)),
            dma((steps, 4)),
            dma((4,)),
            dma((4,)),
        ],
        compiler_params=pltpu.CompilerParams(collective_id=0, has_side_effects=True),
    )(
        velocity, stresses, buoyancy, lame_first, rigidity, histories, mechanism.T, resample.T,
        owners.reshape(1, rows), cell_offsets.reshape(1, rows),
    )
    return pl.pallas_call(
        store_kernel,
        out_shape=(
            jax.ShapeDtypeStruct(velocity.shape, f32),
            jax.ShapeDtypeStruct(stresses.shape, f32),
        ),
        in_specs=[vmem, vmem],
        out_specs=(hbm, hbm),
        scratch_shapes=[dma((3,))],
    )(
        pltpu.with_memory_space_constraint(v_last, pltpu.VMEM),
        pltpu.with_memory_space_constraint(s_last, pltpu.VMEM),
    )


def solution(mesh):
    in_specs = (
        P(None, "gx", "gy", None),
        P(None, "gx", "gy", None),
        P("gx", "gy", None),
        P("gx", "gy", None),
        P("gx", "gy", None),
        P(("gx", "gy"), None),
        P(("gx", "gy"), None),
        P(),
        P(("gx", "gy"), None),
        P(("gx", "gy")),
    )
    out_specs = (P(None, "gx", "gy", None), P(None, "gx", "gy", None))
    return jax.shard_map(local, mesh=mesh, in_specs=in_specs, out_specs=out_specs, check_vma=False)
```

```python
import functools

import jax
import jax.numpy as jnp
from jax import lax
from jax.experimental import pallas as pl
from jax.experimental.pallas import tpu as pltpu
from jax.sharding import PartitionSpec as P

A = 9.0 / 8.0
B = -1.0 / 24.0
MESH = pl.DeviceIdType.MESH
XP = 2
YP = 8

STRESS_FACES = (((0, True), (3, False), (4, False)), ((3, False), (1, True), (5, False)))
VELOCITY_FACES = (((0, False), (1, True), (2, True)), ((0, True), (1, False), (2, True)))


def face_layers(faces, up, extent):
    edge, inward = (extent - 1, -1) if up else (0, 1)
    out, at = [], 0
    for comp, forward in faces:
        wide = forward != up
        out.append((comp, 0, edge, wide, at))
        at += 2 if wide else 1
        if wide:
            out.append((comp, 1, edge + inward, False, at))
            at += 1
    return out


def face_slots(faces, up, extent):
    return sum(2 if wide else 1 for _, _, _, wide, _ in face_layers(faces, up, extent))


def unpacker(faces, up, extent, slot):
    places = {(comp, order): (at, wide) for comp, order, _, wide, at in face_layers(faces, up, extent)}

    def halo(comp, order):
        at, wide = places[comp, order]
        value = slot(at).astype(jnp.float32)
        return value + slot(at + 1).astype(jnp.float32) if wide else value

    return halo


def halo_terms(faces, from_low, extent, halo):
    edge, inward = (0, 1) if from_low else (extent - 1, -1)
    sign = -1.0 if from_low else 1.0
    out = []
    for comp, forward in faces:
        if from_low == forward:
            out.append((comp, 0, edge, sign * B * halo(comp, 0)))
            continue
        first, second = halo(comp, 0), halo(comp, 1)
        out.append((comp, 0, edge, sign * A * first + sign * B * second))
        out.append((comp, 1, edge + inward, sign * B * first))
    return out


def kernel(
    groups, blocks, steps,
    v_hbm, s_hbm, buoy_hbm, lame_hbm, rig_hbm, hist_hbm, mech_hbm, res_hbm, own_hbm, off_hbm,
    v_out, s_out,
    V, S, buoy, lame, rig, hist, mech_ref, res_ref, own_ref, off_ref, src, gathered, plane_hot, level_hot,
    send_x, recv_x, send_y, recv_y, corner_stage, corner_out, corner_in, edge_out_x, edge_in_x, edge_out_y, edge_in_y, edge_x, edge_y, own_x, own_y,
    stress_sem, load_sem, src_send, src_recv, face_send, face_recv,
    corner_send, corner_recv, edge_send, edge_recv,
):
    gx = lax.axis_index("gx")
    gy = lax.axis_index("gy")
    cx, cy, cz = buoy.shape
    rows = hist.shape[0]
    inner = (slice(None), pl.ds(XP, cx), pl.ds(YP, cy), slice(None))

    barrier = pltpu.get_barrier_semaphore()
    sides = (
        (gx > 0, (gx - 1, gy)),
        (gx < blocks - 1, (gx + 1, gy)),
        (gy > 0, (gx, gy - 1)),
        (gy < groups - 1, (gx, gy + 1)),
    )
    for there, device in sides[:2]:
        @pl.when(there)
        def _(device=device):
            pl.semaphore_signal(barrier, inc=1, device_id=device, device_id_type=MESH)
    corners = []
    for ux in range(2):
        for uy in range(2):
            there = jnp.logical_and(sides[ux][0], sides[2 + uy][0])
            corners.append((there, (gx + 2 * ux - 1, gy + 2 * uy - 1)))
    for there, device in corners:
        @pl.when(there)
        def _(device=device):
            pl.semaphore_signal(barrier, inc=1, device_id=device, device_id_type=MESH)
    for k in range(1, groups):
        pl.semaphore_signal(
            barrier, inc=1, device_id=(gx, lax.rem(gy + k, groups)), device_id_type=MESH
        )

    loads = [
        pltpu.make_async_copy(hist_hbm, hist, load_sem.at[0]),
        pltpu.make_async_copy(v_hbm, V.at[inner], load_sem.at[1]),
        pltpu.make_async_copy(buoy_hbm, buoy, load_sem.at[2]),
        pltpu.make_async_copy(lame_hbm, lame, load_sem.at[3]),
        pltpu.make_async_copy(rig_hbm, rig, load_sem.at[4]),
        pltpu.make_async_copy(mech_hbm, mech_ref, load_sem.at[5]),
        pltpu.make_async_copy(res_hbm, res_ref, load_sem.at[6]),
        pltpu.make_async_copy(own_hbm, own_ref, load_sem.at[7]),
        pltpu.make_async_copy(off_hbm, off_ref, load_sem.at[8]),
    ]
    stress_loads = {
        comp: pltpu.make_async_copy(
            s_hbm.at[comp], S.at[(comp,) + inner[1:]], stress_sem.at[comp]
        )
        for comp in (3, 1, 5, 0, 4, 2)
    }
    for load in list(stress_loads.values()) + loads:
        load.start()

    for ref in (V, S):
        zero_x = jnp.zeros((ref.shape[0], XP, cy, cz), jnp.float32)
        ref[:, pl.ds(0, XP), pl.ds(YP, cy), :] = zero_x
        ref[:, pl.ds(XP + cx, XP), pl.ds(YP, cy), :] = zero_x

        def clear(x, carry, ref=ref):
            zero_y = jnp.zeros((ref.shape[0], YP, cz), jnp.float32)
            ref[:, XP + x, pl.ds(0, YP), :] = zero_y
            ref[:, XP + x, pl.ds(YP + cy, YP), :] = zero_y
            return carry

        lax.fori_loop(0, cx, clear, 0)

    def face_copy(phase, side, faces):
        axis, up = side // 2, side % 2
        send, recv = ((send_x, recv_x), (send_y, recv_y))[axis]
        count = face_slots(faces[axis], bool(up), (cx, cy)[axis])
        return pltpu.make_async_remote_copy(
            src_ref=send.at[phase, up, pl.ds(0, count)],
            dst_ref=recv.at[phase, up, pl.ds(0, count)],
            send_sem=face_send.at[phase, side],
            recv_sem=face_recv.at[phase, side],
            device_id=sides[side][1],
            device_id_type=MESH,
        )

    def row(ref, comp, axis, layer):
        x, y = (XP, YP) if ref is V or ref is S else (0, 0)
        if axis == 0:
            return ref.at[comp, x + layer, pl.ds(y, cy), :]
        return ref.at[comp, pl.ds(x, cx), y + layer, :]

    def coefficient(ref, axis, layer):
        return ref[layer] if axis == 0 else ref[:, layer, :]

    odd = lax.rem(gy, 2) == 1
    even = jnp.logical_not(odd)
    near = ((2, jnp.logical_and(sides[2][0], odd)), (3, jnp.logical_and(sides[3][0], even)))
    far = ((3, jnp.logical_and(sides[3][0], odd)), (2, jnp.logical_and(sides[2][0], even)))
    across = ((0, sides[0][0]), (1, sides[1][0]))

    def send_face(side, phase, ref, faces):
        axis, up = side // 2, side % 2
        send = (send_x, send_y)[axis]
        for comp, _, layer, wide, at in face_layers(faces[axis], bool(up), (cx, cy)[axis]):
            value = row(ref, comp, axis, layer)[...]
            head = value.astype(jnp.bfloat16)
            send[phase, up, at] = head
            if wide:
                rest = value - head.astype(jnp.float32)
                send[phase, up, at + 1] = rest.astype(jnp.bfloat16)
        face_copy(phase, side, faces).start()

    def receive_face(side, phase, faces, apply, partial=None):
        axis, up = side // 2, side % 2
        extent = (cx, cy)[axis]
        recv = (recv_x, recv_y)[axis]
        face_copy(phase, 2 * axis + 1 - up, faces).wait_recv()
        arrived = unpacker(faces[axis], not up, extent, lambda at: recv[phase, 1 - up, at])
        halo = arrived if partial is None else lambda comp, order: arrived(comp, order) + partial(side, comp, order)
        for comp, _, layer, value in halo_terms(faces[axis], not up, extent, halo):
            apply(axis, comp, layer, value)

    def edge_copy(side):
        axis, up = side // 2, side % 2
        out, into = ((edge_out_x, edge_in_x), (edge_out_y, edge_in_y))[axis]
        return pltpu.make_async_remote_copy(
            src_ref=out.at[up], dst_ref=into.at[up],
            send_sem=edge_send.at[side], recv_sem=edge_recv.at[side],
            device_id=sides[side][1], device_id_type=MESH,
        )

    def send_edge(side):
        axis, up = side // 2, side % 2
        extent, out = (cx, cy)[axis], (edge_out_x, edge_out_y)[axis]
        near = coefficient(buoy, axis, extent - 1 if up else 0)
        head = near.astype(jnp.bfloat16)
        out[up, 0] = head
        out[up, 1] = (near - head.astype(jnp.float32)).astype(jnp.bfloat16)
        out[up, 2] = coefficient(buoy, axis, extent - 2 if up else 1).astype(jnp.bfloat16)
        edge_copy(side).start()

    def receive_edge(side):
        axis, up = side // 2, side % 2
        into = (edge_in_x, edge_in_y)[axis]
        edge_copy(2 * axis + 1 - up).wait_recv()
        arrived = [into[1 - up, k].astype(jnp.float32) for k in range(3)]
        edges[axis][1 - up, 0] = arrived[0] + arrived[1]
        edges[axis][1 - up, 1] = arrived[2]

    velocity_places = [
        [
            {(comp, order): k for k, (comp, order, *_) in enumerate(face_layers(VELOCITY_FACES[axis], not up, extent))}
            for up in (False, True)
        ]
        for axis, extent in enumerate((cx, cy))
    ]
    force_of = ({0: 0, 3: 1, 4: 2}, {3: 0, 1: 1, 5: 2})
    owns, edges = (own_x, own_y), (edge_x, edge_y)

    def own_part(side, phase):
        axis, up = side // 2, side % 2
        send = (send_x, send_y)[axis]
        halo = unpacker(STRESS_FACES[axis], bool(up), (cx, cy)[axis], lambda at: send[phase, up, at])
        for comp, order, _, value in halo_terms(STRESS_FACES[axis], bool(up), (cx, cy)[axis], halo):
            k = velocity_places[axis][up][force_of[axis][comp], order]
            factor = edges[axis][1 - up, order]
            owns[axis][up, k] = factor * value

    def partial_velocity(side, comp, order):
        axis, up = side // 2, side % 2
        return owns[axis][up, velocity_places[axis][up][comp, order]]

    def corner_terms(ups):
        out = []
        for axis in range(2):
            other = 1 - axis
            for (vcomp, order), k in velocity_places[axis][ups[axis]].items():
                faces = [f for f in STRESS_FACES[other] if force_of[other][f[0]] == vcomp]
                out.append((axis, k, order, faces))
        return out

    def corner_rows(ups):
        rows = {}
        for axis, _, order, faces in corner_terms(ups):
            def halo(comp, across, axis=axis, order=order):
                rows.setdefault((comp, order, across) if axis == 0 else (comp, across, order), len(rows))
                return 0.0
            halo_terms(faces, not ups[1 - axis], (cx, cy)[1 - axis], halo)
        return rows

    def corner_copy(t, corner):
        return pltpu.make_async_remote_copy(
            src_ref=corner_out.at[t, corner], dst_ref=corner_in.at[t, corner],
            send_sem=corner_send.at[t, corner], recv_sem=corner_recv.at[t, corner],
            device_id=corners[corner][1], device_id_type=MESH,
        )

    def send_corner(t, corner):
        ux, uy = corner // 2, corner % 2
        for (comp, xo, yo), r in corner_rows((1 - ux, 1 - uy)).items():
            x, y = cx - 1 - xo if ux else xo, cy - 1 - yo if uy else yo
            corner_stage[corner, pl.ds(r, 1), :] = S[comp, XP + x, pl.ds(YP + y, 1), :]
        corner_out[t, corner] = corner_stage[corner].astype(jnp.bfloat16)
        corner_copy(t, corner).start()

    def receive_corner(t, corner):
        ups = (corner // 2, corner % 2)
        corner_copy(t, 3 - corner).wait_recv()
        rows = corner_rows(ups)
        arrived = corner_in[t, 3 - corner].astype(jnp.float32)
        for axis, k, order, faces in corner_terms(ups):
            up = ups[axis]

            def halo(comp, across):
                r = rows[(comp, order, across) if axis == 0 else (comp, across, order)]
                return arrived[r : r + 1]

            for _, _, layer, value in halo_terms(faces, not ups[1 - axis], (cx, cy)[1 - axis], halo):
                place = owns[axis].at[up, k, pl.ds(layer, 1), :]
                place[...] = place[...] + edges[axis][1 - up, order, pl.ds(layer, 1), :] * value

    def at_corners(*actions):
        for corner, (there, _) in enumerate(corners):
            @pl.when(there)
            def _(corner=corner):
                for action in actions:
                    action(corner)

    def at_sides(which, *actions):
        for side, there in which:
            @pl.when(there)
            def _(side=side):
                for action in actions:
                    action(side)

    def finish_faces(phase, faces):
        for side in (0, 1, 2, 3):
            @pl.when(sides[side][0])
            def _(side=side):
                face_copy(phase, side, faces).wait_send()

    def add(ref, comp, axis, layer, value):
        place = row(ref, comp, axis, layer)
        place[...] = place[...] + value

    def apply_force(axis, comp, layer, value):
        add(V, force_of[axis][comp], axis, layer, coefficient(buoy, axis, layer) * value)

    shear_of = ({1: 3, 2: 4}, {0: 3, 2: 5})

    def apply_strain(target, axis, comp, layer, value):
        mu = coefficient(rig, axis, layer)
        if comp != axis:
            add(target, shear_of[axis][comp], axis, layer, mu * value)
            return
        volume = coefficient(lame, axis, layer) * value
        for normal in range(3):
            extra = volume + 2.0 * mu * value if normal == axis else volume
            add(target, normal, axis, layer, extra)

    level = lax.broadcasted_iota(jnp.int32, (cy, cz), 1)

    def along_z(values, by):
        moved = pltpu.roll(values, (-by) % cz, 1)
        return jnp.where(level < cz - by if by > 0 else level >= -by, moved, 0.0)

    def differ(ref, comp, x, dimension, forward):
        def window(by):
            if dimension == 0:
                return ref[comp, XP + x + by, pl.ds(YP, cy), :]
            if dimension == 1:
                return ref[comp, XP + x, pl.ds(YP + by, cy), :]
            values = ref[comp, XP + x, pl.ds(YP, cy), :]
            return along_z(values, by) if by else values

        if forward:
            return A * (window(1) - window(0)) + B * (window(2) - window(-1))
        return A * (window(0) - window(-1)) + B * (window(1) - window(-2))

    def velocity_inner(x, carry):
        force = (
            differ(S, 0, x, 0, True) + differ(S, 3, x, 1, False) + differ(S, 4, x, 2, False),
            differ(S, 3, x, 0, False) + differ(S, 1, x, 1, True) + differ(S, 5, x, 2, False),
            differ(S, 4, x, 0, False) + differ(S, 5, x, 1, False) + differ(S, 2, x, 2, True),
        )
        factor = buoy[x]
        for comp in range(3):
            place = V.at[comp, XP + x, pl.ds(YP, cy), :]
            place[...] = place[...] + factor * force[comp]
        return carry

    def stress_inner(last, x, carry):
        one = differ(V, 0, x, 0, False)
        two = differ(V, 1, x, 1, False)
        three = differ(V, 2, x, 2, False)
        mu = rig[x]
        volume = lame[x] * (one + two + three)
        rates = (
            volume + 2.0 * mu * one,
            volume + 2.0 * mu * two,
            volume + 2.0 * mu * three,
            mu * (differ(V, 0, x, 1, True) + differ(V, 1, x, 0, True)),
            mu * (differ(V, 0, x, 2, True) + differ(V, 2, x, 0, True)),
            mu * (differ(V, 1, x, 2, True) + differ(V, 2, x, 1, True)),
        )
        for comp in range(6):
            place = S.at[comp, XP + x, pl.ds(YP, cy), :]
            target = s_out.at[comp, x] if last else place
            target[...] = place[...] + rates[comp]
        if last:
            for comp in range(3):
                v_out[comp, x] = V[comp, XP + x, pl.ds(YP, cy), :]
        return carry

    def sweep(body):
        batch = max(b for b in (8, 4, 2, 1) if cx % b == 0)

        def several(at, carry):
            for one in range(batch):
                carry = body(batch * at + one, carry)
            return carry

        lax.fori_loop(0, cx // batch, several, 0)

    def source_copy(k):
        return pltpu.make_async_remote_copy(
            src_ref=src,
            dst_ref=gathered.at[:, pl.ds(k * rows, rows)],
            send_sem=src_send.at[k],
            recv_sem=src_recv.at[k],
            device_id=(gx, lax.rem(gy + k, groups)),
            device_id_type=MESH,
        )

    comps = src.shape[0] // (steps + 1)

    def source_terms():
        contract_last = (((1,), (1,)), ((), ()))
        amplitude = lax.dot_general(
            res_ref[...], hist[...], contract_last, preferred_element_type=jnp.float32
        )
        mech = mech_ref[...].astype(jnp.float32)
        spare = jnp.zeros((comps - mech.shape[0], rows), jnp.float32)
        parts = []
        for t in range(steps):
            parts += [mech * amplitude[t : t + 1, :], spare]
        offsets = off_ref[...]
        places = [own_ref[...], offsets // (cy * cz), (offsets // cz) % cy, offsets % cz]
        places = [p.astype(jnp.float32) for p in places]
        parts += [jnp.concatenate(places + [jnp.zeros((comps - 4, rows), jnp.float32)], axis=0)]
        packed = jnp.concatenate(parts, axis=0).astype(jnp.bfloat16)
        src[...] = packed
        gathered[:, pl.ds(0, rows)] = packed

    def source_masks():
        for k in range(groups):
            lanes = pl.ds(k * rows, rows)
            info = gathered[pl.ds(steps * comps, comps), lanes].astype(jnp.float32)
            cell_plane = info[0:1] * float(cx * cy) + info[1:2] * float(cy) + info[2:3]
            plane = lax.broadcasted_iota(jnp.int32, (cx * cy, rows), 0) + gy * (cx * cy)
            plane_hot[:, lanes] = jnp.where(
                plane == cell_plane.astype(jnp.int32), 1.0, 0.0
            ).astype(jnp.bfloat16)
            height = lax.broadcasted_iota(jnp.int32, (cz, rows), 0)
            level_hot[:, lanes] = jnp.where(
                height == info[3:4].astype(jnp.int32), 1.0, 0.0
            ).astype(jnp.bfloat16)

    def insert_sources(t):
        values = gathered[pl.ds(t * comps, comps), :].astype(jnp.float32)
        for comp in range(0, 6, 2):
            spread = jnp.concatenate(
                [
                    level_hot[...] * values[c : c + 1, :].astype(jnp.bfloat16)
                    for c in (comp, comp + 1)
                ],
                axis=0,
            )
            placed = lax.dot_general(
                plane_hot[...], spread, (((1,), (1,)), ((), ())),
                preferred_element_type=jnp.float32,
            )
            for c in range(2):
                place = S.at[comp + c, pl.ds(XP, cx), pl.ds(YP, cy), :]
                place[...] = place[...] + placed[:, c * cz : (c + 1) * cz].reshape(cx, cy, cz)

    arrivals = groups - 1
    for there, _ in list(sides[:2]) + corners:
        arrivals += there.astype(jnp.int32)

    def send_stress(t):
        def send(side):
            send_face(side, 2 * t, S, STRESS_FACES)

        at_sides(far, send)
        at_sides(near, send)
        at_corners(functools.partial(send_corner, t))
        at_sides(across, send)

    corner_stage[...] = jnp.zeros_like(corner_stage)
    pl.semaphore_wait(barrier, arrivals)
    for load in stress_loads.values():
        load.wait()
    send_stress(0)
    for load in [loads[0]] + loads[5:]:
        load.wait()
    source_terms()
    for k in range(1, groups):
        source_copy(k).start()
    loads[1].wait()
    loads[2].wait()
    everywhere = far + near + across
    for t in range(steps):
        first, second = 2 * t, 2 * t + 1
        last = t == steps - 1
        sweep(velocity_inner)
        at_sides(everywhere, lambda side: send_face(side, second, V, VELOCITY_FACES))
        if t == 0:
            at_sides(everywhere, send_edge)
        else:
            at_sides(everywhere, lambda side: own_part(side, first))
            insert_sources(t)
        at_sides(across + near + far, lambda side: receive_face(side, first, STRESS_FACES, apply_force))
        if t == 0:
            loads[3].wait()
            loads[4].wait()
            if last:
                for k in range(1, groups):
                    source_copy(k).wait_recv()
                source_masks()
                insert_sources(0)
        sweep(functools.partial(stress_inner, last))
        if t == 0 and not last:
            for k in range(1, groups):
                source_copy(k).wait_recv()
            source_masks()
            insert_sources(0)
        if t == 0:
            at_sides(across + near + far, receive_edge, lambda side: own_part(side, first))
        at_corners(functools.partial(receive_corner, t))
        strain = functools.partial(apply_strain, s_out if last else S)
        at_sides(
            across + near + far,
            lambda side: receive_face(side, second, VELOCITY_FACES, strain, partial_velocity),
        )
        if not last:
            send_stress(t + 1)
    for t in range(steps):
        finish_faces(2 * t, STRESS_FACES)
        finish_faces(2 * t + 1, VELOCITY_FACES)
        at_corners(lambda corner: corner_copy(t, corner).wait_send())
    at_sides(everywhere, lambda side: edge_copy(side).wait_send())
    for k in range(1, groups):
        source_copy(k).wait_send()


def store_kernel(v_ref, s_ref, v_out, s_out, sem):
    copies = [pltpu.make_async_copy(v_ref, v_out, sem.at[0])]
    half = s_ref.shape[0] // 2
    for part in range(2):
        layers = pl.ds(part * half, half)
        copies.append(pltpu.make_async_copy(s_ref.at[layers], s_out.at[layers], sem.at[1 + part]))
    for copy in copies:
        copy.start()
    for copy in copies:
        copy.wait()


def local(
    velocity, stresses, buoyancy, lame_first, rigidity,
    histories, mechanism, resample, owners, cell_offsets,
):
    groups = lax.axis_size("gy")
    blocks = lax.axis_size("gx")
    rows, samples = histories.shape
    steps = resample.shape[1]
    _, cx, cy, cz = velocity.shape
    comps = 8
    tall = comps * (steps + 1)
    f32, bf16 = jnp.float32, jnp.bfloat16
    hbm = pl.BlockSpec(memory_space=pl.ANY)
    vmem = pl.BlockSpec(memory_space=pltpu.VMEM)
    dma = pltpu.SemaphoreType.DMA
    phases = 2 * steps
    v_last, s_last = pl.pallas_call(
        functools.partial(kernel, groups, blocks, steps),
        out_shape=(
            pltpu.VMEM(velocity.shape, f32),
            pltpu.VMEM(stresses.shape, f32),
        ),
        in_specs=[hbm] * 10,
        out_specs=(vmem, vmem),
        scratch_shapes=[
            pltpu.VMEM((3, cx + 2 * XP, cy + 2 * YP, cz), f32),
            pltpu.VMEM((6, cx + 2 * XP, cy + 2 * YP, cz), f32),
            pltpu.VMEM((cx, cy, cz), f32),
            pltpu.VMEM((cx, cy, cz), f32),
            pltpu.VMEM((cx, cy, cz), f32),
            pltpu.VMEM((rows, samples), bf16),
            pltpu.VMEM((mechanism.shape[1], rows), bf16),
            pltpu.VMEM((steps, samples), bf16),
            pltpu.VMEM((1, rows), jnp.int32),
            pltpu.VMEM((1, rows), jnp.int32),
            pltpu.VMEM((tall, rows), bf16),
            pltpu.VMEM((tall, groups * rows), bf16),
            pltpu.VMEM((cx * cy, groups * rows), bf16),
            pltpu.VMEM((cz, groups * rows), bf16),
            pltpu.VMEM((phases, 2, 9, cy, cz), bf16),
            pltpu.VMEM((phases, 2, 9, cy, cz), bf16),
            pltpu.VMEM((phases, 2, 9, cx, cz), bf16),
            pltpu.VMEM((phases, 2, 9, cx, cz), bf16),
            pltpu.VMEM((4, 16, cz), f32),
            pltpu.VMEM((steps, 4, 16, cz), bf16),
            pltpu.VMEM((steps, 4, 16, cz), bf16),
            pltpu.VMEM((2, 3, cy, cz), bf16),
            pltpu.VMEM((2, 3, cy, cz), bf16),
            pltpu.VMEM((2, 3, cx, cz), bf16),
            pltpu.VMEM((2, 3, cx, cz), bf16),
            pltpu.VMEM((2, 2, cy, cz), f32),
            pltpu.VMEM((2, 2, cx, cz), f32),
            pltpu.VMEM((2, 5, cy, cz), f32),
            pltpu.VMEM((2, 5, cx, cz), f32),
            dma((6,)),
            dma((9,)),
            dma((groups,)),
            dma((groups,)),
            dma((phases, 4)),
            dma((phases, 4)),
            dma((steps, 4)),
            dma((steps, 4)),
            dma((4,)),
            dma((4,)),
        ],
        compiler_params=pltpu.CompilerParams(collective_id=0, has_side_effects=True),
    )(
        velocity, stresses, buoyancy, lame_first, rigidity, histories, mechanism.T, resample.T,
        owners.reshape(1, rows), cell_offsets.reshape(1, rows),
    )
    return pl.pallas_call(
        store_kernel,
        out_shape=(
            jax.ShapeDtypeStruct(velocity.shape, f32),
            jax.ShapeDtypeStruct(stresses.shape, f32),
        ),
        in_specs=[vmem, vmem],
        out_specs=(hbm, hbm),
        scratch_shapes=[dma((3,))],
    )(
        pltpu.with_memory_space_constraint(v_last, pltpu.VMEM),
        pltpu.with_memory_space_constraint(s_last, pltpu.VMEM),
    )


def solution(mesh):
    in_specs = (
        P(None, "gx", "gy", None),
        P(None, "gx", "gy", None),
        P("gx", "gy", None),
        P("gx", "gy", None),
        P("gx", "gy", None),
        P(("gx", "gy"), None),
        P(("gx", "gy"), None),
        P(),
        P(("gx", "gy"), None),
        P(("gx", "gy")),
    )
    out_specs = (P(None, "gx", "gy", None), P(None, "gx", "gy", None))
    return jax.shard_map(local, mesh=mesh, in_specs=in_specs, out_specs=out_specs, check_vma=False)
```

```python
import functools

import jax
import jax.numpy as jnp
from jax import lax
from jax.experimental import pallas as pl
from jax.experimental.pallas import tpu as pltpu
from jax.sharding import PartitionSpec as P

A = 9.0 / 8.0
B = -1.0 / 24.0
MESH = pl.DeviceIdType.MESH
XP = 2
YP = 8
CAP = 64
BUOYANCY = (0.45, 0.15 / 32767.0)

STRESS_FACES = (((0, True), (3, False), (4, False)), ((3, False), (1, True), (5, False)))
VELOCITY_FACES = (((0, False), (1, True), (2, True)), ((0, True), (1, False), (2, True)))


def face_layers(faces, up, extent):
    edge, inward = (extent - 1, -1) if up else (0, 1)
    out, at = [], 0
    for comp, forward in faces:
        wide = forward != up
        out.append((comp, 0, edge, wide, at))
        at += 2 if wide else 1
        if wide:
            out.append((comp, 1, edge + inward, False, at))
            at += 1
    return out


def face_slots(faces, up, extent):
    return sum(2 if wide else 1 for _, _, _, wide, _ in face_layers(faces, up, extent))


def unpacker(faces, up, extent, slot):
    places = {(comp, order): (at, wide) for comp, order, _, wide, at in face_layers(faces, up, extent)}

    def halo(comp, order):
        at, wide = places[comp, order]
        value = slot(at).astype(jnp.float32)
        return value + slot(at + 1).astype(jnp.float32) if wide else value

    return halo


def halo_terms(faces, from_low, extent, halo):
    edge, inward = (0, 1) if from_low else (extent - 1, -1)
    sign = -1.0 if from_low else 1.0
    out = []
    for comp, forward in faces:
        if from_low == forward:
            out.append((comp, 0, edge, sign * B * halo(comp, 0)))
            continue
        first, second = halo(comp, 0), halo(comp, 1)
        out.append((comp, 0, edge, sign * A * first + sign * B * second))
        out.append((comp, 1, edge + inward, sign * B * first))
    return out


def kernel(
    groups, blocks, steps,
    v_hbm, s_hbm, buoy_hbm, lame_hbm, rig_hbm, hist_hbm, mech_hbm, res_hbm, own_hbm, off_hbm,
    v_out, s_out,
    V, S, buoy, lame, rig, hist, mech_ref, res_ref, own_ref, off_ref, select, src, gathered, values, plane_hot, level_hot,
    send_x, recv_x, send_y, recv_y, corner_stage, corner_out, corner_in, edge_out_x, edge_in_x, edge_out_y, edge_in_y, edge_x, edge_y, own_x, own_y,
    stress_sem, load_sem, src_send, src_recv, face_send, face_recv,
    corner_send, corner_recv, edge_send, edge_recv,
):
    gx = lax.axis_index("gx")
    gy = lax.axis_index("gy")
    cx, cy, cz = buoy.shape
    rows = hist.shape[0]
    inner = (slice(None), pl.ds(XP, cx), pl.ds(YP, cy), slice(None))

    barrier = pltpu.get_barrier_semaphore()
    sides = (
        (gx > 0, (gx - 1, gy)),
        (gx < blocks - 1, (gx + 1, gy)),
        (gy > 0, (gx, gy - 1)),
        (gy < groups - 1, (gx, gy + 1)),
    )
    for there, device in sides[:2]:
        @pl.when(there)
        def _(device=device):
            pl.semaphore_signal(barrier, inc=1, device_id=device, device_id_type=MESH)
    corners = []
    for ux in range(2):
        for uy in range(2):
            there = jnp.logical_and(sides[ux][0], sides[2 + uy][0])
            corners.append((there, (gx + 2 * ux - 1, gy + 2 * uy - 1)))
    for there, device in corners:
        @pl.when(there)
        def _(device=device):
            pl.semaphore_signal(barrier, inc=1, device_id=device, device_id_type=MESH)
    for k in range(1, groups):
        pl.semaphore_signal(
            barrier, inc=1, device_id=(gx, lax.rem(gy + k, groups)), device_id_type=MESH
        )

    loads = [
        pltpu.make_async_copy(hist_hbm, hist, load_sem.at[0]),
        pltpu.make_async_copy(v_hbm, V.at[inner], load_sem.at[1]),
        pltpu.make_async_copy(buoy_hbm, buoy, load_sem.at[2]),
        pltpu.make_async_copy(lame_hbm, lame, load_sem.at[3]),
        pltpu.make_async_copy(rig_hbm, rig, load_sem.at[4]),
        pltpu.make_async_copy(mech_hbm, mech_ref, load_sem.at[5]),
        pltpu.make_async_copy(res_hbm, res_ref, load_sem.at[6]),
        pltpu.make_async_copy(own_hbm, own_ref, load_sem.at[7]),
        pltpu.make_async_copy(off_hbm, off_ref, load_sem.at[8]),
    ]
    stress_loads = {
        comp: pltpu.make_async_copy(
            s_hbm.at[comp], S.at[(comp,) + inner[1:]], stress_sem.at[comp]
        )
        for comp in (3, 1, 5, 0, 4, 2)
    }
    for load in [loads[7]] + list(stress_loads.values()) + loads[:7] + loads[8:]:
        load.start()

    for ref in (V, S):
        zero_x = jnp.zeros((ref.shape[0], XP, cy, cz), jnp.float32)
        ref[:, pl.ds(0, XP), pl.ds(YP, cy), :] = zero_x
        ref[:, pl.ds(XP + cx, XP), pl.ds(YP, cy), :] = zero_x

        def clear(x, carry, ref=ref):
            zero_y = jnp.zeros((ref.shape[0], YP, cz), jnp.float32)
            ref[:, XP + x, pl.ds(0, YP), :] = zero_y
            ref[:, XP + x, pl.ds(YP + cy, YP), :] = zero_y
            return carry

        lax.fori_loop(0, cx, clear, 0)

    def face_copy(phase, side, faces):
        axis, up = side // 2, side % 2
        send, recv = ((send_x, recv_x), (send_y, recv_y))[axis]
        count = face_slots(faces[axis], bool(up), (cx, cy)[axis])
        return pltpu.make_async_remote_copy(
            src_ref=send.at[phase, up, pl.ds(0, count)],
            dst_ref=recv.at[phase, up, pl.ds(0, count)],
            send_sem=face_send.at[phase, side],
            recv_sem=face_recv.at[phase, side],
            device_id=sides[side][1],
            device_id_type=MESH,
        )

    def row(ref, comp, axis, layer):
        x, y = (XP, YP) if ref is V or ref is S else (0, 0)
        if axis == 0:
            return ref.at[comp, x + layer, pl.ds(y, cy), :]
        _, planes, height, _ = ref.shape
        flat = ref.reshape(ref.shape[0], planes * height, cz)
        return flat.at[comp, pl.ds(x * height + y + layer, cx, stride=height), :]

    def coefficient(ref, axis, layer):
        return ref[layer] if axis == 0 else ref[:, layer, :]

    odd = lax.rem(gy, 2) == 1
    even = jnp.logical_not(odd)
    near = ((2, jnp.logical_and(sides[2][0], odd)), (3, jnp.logical_and(sides[3][0], even)))
    far = ((3, jnp.logical_and(sides[3][0], odd)), (2, jnp.logical_and(sides[2][0], even)))
    across = ((0, sides[0][0]), (1, sides[1][0]))

    def send_face(side, phase, ref, faces):
        axis, up = side // 2, side % 2
        send = (send_x, send_y)[axis]
        for comp, _, layer, wide, at in face_layers(faces[axis], bool(up), (cx, cy)[axis]):
            value = row(ref, comp, axis, layer)[...]
            head = value.astype(jnp.bfloat16)
            send[phase, up, at] = head
            if wide:
                rest = value - head.astype(jnp.float32)
                send[phase, up, at + 1] = rest.astype(jnp.bfloat16)
        face_copy(phase, side, faces).start()

    def receive_face(side, phase, faces, apply, partial=None):
        axis, up = side // 2, side % 2
        extent = (cx, cy)[axis]
        recv = (recv_x, recv_y)[axis]
        face_copy(phase, 2 * axis + 1 - up, faces).wait_recv()
        arrived = unpacker(faces[axis], not up, extent, lambda at: recv[phase, 1 - up, at])
        halo = arrived if partial is None else lambda comp, order: arrived(comp, order) + partial(side, comp, order)
        for comp, _, layer, value in halo_terms(faces[axis], not up, extent, halo):
            apply(axis, comp, layer, value)

    def edge_copy(side):
        axis, up = side // 2, side % 2
        out, into = ((edge_out_x, edge_in_x), (edge_out_y, edge_in_y))[axis]
        return pltpu.make_async_remote_copy(
            src_ref=out.at[up], dst_ref=into.at[up],
            send_sem=edge_send.at[side], recv_sem=edge_recv.at[side],
            device_id=sides[side][1], device_id_type=MESH,
        )

    def send_edge(side):
        axis, up = side // 2, side % 2
        extent, out = (cx, cy)[axis], (edge_out_x, edge_out_y)[axis]
        middle, grain = BUOYANCY
        for order in range(2):
            value = coefficient(buoy, axis, extent - 1 - order if up else order)
            coded = jnp.clip(jnp.round((value - middle) * (1.0 / grain)), -32767.0, 32767.0)
            out[up, order] = coded.astype(jnp.int32).astype(jnp.int16)
        edge_copy(side).start()

    def receive_edge(side):
        axis, up = side // 2, side % 2
        into = (edge_in_x, edge_in_y)[axis]
        edge_copy(2 * axis + 1 - up).wait_recv()
        middle, grain = BUOYANCY
        for order in range(2):
            edges[axis][1 - up, order] = into[1 - up, order].astype(jnp.int32).astype(jnp.float32) * grain + middle

    velocity_places = [
        [
            {(comp, order): k for k, (comp, order, *_) in enumerate(face_layers(VELOCITY_FACES[axis], not up, extent))}
            for up in (False, True)
        ]
        for axis, extent in enumerate((cx, cy))
    ]
    force_of = ({0: 0, 3: 1, 4: 2}, {3: 0, 1: 1, 5: 2})
    owns, edges = (own_x, own_y), (edge_x, edge_y)

    def own_part(side, phase):
        axis, up = side // 2, side % 2
        send = (send_x, send_y)[axis]
        halo = unpacker(STRESS_FACES[axis], bool(up), (cx, cy)[axis], lambda at: send[phase, up, at])
        for comp, order, _, value in halo_terms(STRESS_FACES[axis], bool(up), (cx, cy)[axis], halo):
            k = velocity_places[axis][up][force_of[axis][comp], order]
            factor = edges[axis][1 - up, order]
            owns[axis][up, k] = factor * value

    def partial_velocity(side, comp, order):
        axis, up = side // 2, side % 2
        return owns[axis][up, velocity_places[axis][up][comp, order]]

    def corner_terms(ups):
        out = []
        for axis in range(2):
            other = 1 - axis
            for (vcomp, order), k in velocity_places[axis][ups[axis]].items():
                faces = [f for f in STRESS_FACES[other] if force_of[other][f[0]] == vcomp]
                out.append((axis, k, order, faces))
        return out

    def corner_rows(ups):
        rows = {}
        for axis, _, order, faces in corner_terms(ups):
            def halo(comp, across, axis=axis, order=order):
                rows.setdefault((comp, order, across) if axis == 0 else (comp, across, order), len(rows))
                return 0.0
            halo_terms(faces, not ups[1 - axis], (cx, cy)[1 - axis], halo)
        return rows

    def corner_copy(t, corner):
        return pltpu.make_async_remote_copy(
            src_ref=corner_out.at[t, corner], dst_ref=corner_in.at[t, corner],
            send_sem=corner_send.at[t, corner], recv_sem=corner_recv.at[t, corner],
            device_id=corners[corner][1], device_id_type=MESH,
        )

    def send_corner(t, corner):
        ux, uy = corner // 2, corner % 2
        for (comp, xo, yo), r in corner_rows((1 - ux, 1 - uy)).items():
            x, y = cx - 1 - xo if ux else xo, cy - 1 - yo if uy else yo
            corner_stage[corner, pl.ds(r, 1), :] = S[comp, XP + x, pl.ds(YP + y, 1), :]
        corner_out[t, corner] = corner_stage[corner].astype(jnp.bfloat16)
        corner_copy(t, corner).start()

    def receive_corner(t, corner):
        ups = (corner // 2, corner % 2)
        corner_copy(t, 3 - corner).wait_recv()
        rows = corner_rows(ups)
        arrived = corner_in[t, 3 - corner].astype(jnp.float32)
        for axis, k, order, faces in corner_terms(ups):
            up = ups[axis]

            def halo(comp, across):
                r = rows[(comp, order, across) if axis == 0 else (comp, across, order)]
                return arrived[r : r + 1]

            for _, _, layer, value in halo_terms(faces, not ups[1 - axis], (cx, cy)[1 - axis], halo):
                place = owns[axis].at[up, k, pl.ds(layer, 1), :]
                place[...] = place[...] + edges[axis][1 - up, order, pl.ds(layer, 1), :] * value

    def at_corners(*actions):
        for corner, (there, _) in enumerate(corners):
            @pl.when(there)
            def _(corner=corner):
                for action in actions:
                    action(corner)

    def at_sides(which, *actions):
        for side, there in which:
            @pl.when(there)
            def _(side=side):
                for action in actions:
                    action(side)

    def finish_faces(phase, faces):
        for side in (0, 1, 2, 3):
            @pl.when(sides[side][0])
            def _(side=side):
                face_copy(phase, side, faces).wait_send()

    def add(ref, comp, axis, layer, value):
        place = row(ref, comp, axis, layer)
        place[...] = place[...] + value

    def apply_force(axis, comp, layer, value):
        add(V, force_of[axis][comp], axis, layer, coefficient(buoy, axis, layer) * value)

    shear_of = ({1: 3, 2: 4}, {0: 3, 2: 5})

    def apply_strain(target, axis, comp, layer, value):
        mu = coefficient(rig, axis, layer)
        if comp != axis:
            add(target, shear_of[axis][comp], axis, layer, mu * value)
            return
        volume = coefficient(lame, axis, layer) * value
        for normal in range(3):
            extra = volume + 2.0 * mu * value if normal == axis else volume
            add(target, normal, axis, layer, extra)

    level = lax.broadcasted_iota(jnp.int32, (cy, cz), 1)

    def along_z(values, by):
        moved = pltpu.roll(values, (-by) % cz, 1)
        return jnp.where(level < cz - by if by > 0 else level >= -by, moved, 0.0)

    def differ(ref, comp, x, dimension, forward):
        def window(by):
            if dimension == 0:
                return ref[comp, XP + x + by, pl.ds(YP, cy), :]
            if dimension == 1:
                return ref[comp, XP + x, pl.ds(YP + by, cy), :]
            values = ref[comp, XP + x, pl.ds(YP, cy), :]
            return along_z(values, by) if by else values

        if forward:
            return A * (window(1) - window(0)) + B * (window(2) - window(-1))
        return A * (window(0) - window(-1)) + B * (window(1) - window(-2))

    def velocity_inner(x, carry):
        force = (
            differ(S, 0, x, 0, True) + differ(S, 3, x, 1, False) + differ(S, 4, x, 2, False),
            differ(S, 3, x, 0, False) + differ(S, 1, x, 1, True) + differ(S, 5, x, 2, False),
            differ(S, 4, x, 0, False) + differ(S, 5, x, 1, False) + differ(S, 2, x, 2, True),
        )
        factor = buoy[x]
        for comp in range(3):
            place = V.at[comp, XP + x, pl.ds(YP, cy), :]
            place[...] = place[...] + factor * force[comp]
        return carry

    def stress_inner(last, x, carry):
        one = differ(V, 0, x, 0, False)
        two = differ(V, 1, x, 1, False)
        three = differ(V, 2, x, 2, False)
        mu = rig[x]
        volume = lame[x] * (one + two + three)
        rates = (
            volume + 2.0 * mu * one,
            volume + 2.0 * mu * two,
            volume + 2.0 * mu * three,
            mu * (differ(V, 0, x, 1, True) + differ(V, 1, x, 0, True)),
            mu * (differ(V, 0, x, 2, True) + differ(V, 2, x, 0, True)),
            mu * (differ(V, 1, x, 2, True) + differ(V, 2, x, 1, True)),
        )
        for comp in range(6):
            place = S.at[comp, XP + x, pl.ds(YP, cy), :]
            target = s_out.at[comp, x] if last else place
            target[...] = place[...] + rates[comp]
        if last:
            for comp in range(3):
                v_out[comp, x] = V[comp, XP + x, pl.ds(YP, cy), :]
        return carry

    def sweep(body):
        batch = max(b for b in (8, 4, 2, 1) if cx % b == 0)

        def several(at, carry):
            for one in range(batch):
                carry = body(batch * at + one, carry)
            return carry

        lax.fori_loop(0, cx // batch, several, 0)

    def source_copy(k):
        owner = lax.rem(gy + k, groups)
        return pltpu.make_async_remote_copy(
            src_ref=src.at[owner],
            dst_ref=gathered.at[k],
            send_sem=src_send.at[k],
            recv_sem=src_recv.at[k],
            device_id=(gx, owner),
            device_id_type=MESH,
        )

    comps = 8
    tall = src.shape[1]
    contract_last = (((1,), (1,)), ((), ()))

    def source_slots():
        own = own_ref[...]
        padded = -(-groups // 16) * 16
        mine = (lax.broadcasted_iota(jnp.int32, (padded, rows), 0) == own).astype(jnp.float32)
        before = lax.broadcasted_iota(jnp.int32, (rows, rows), 0) <= lax.broadcasted_iota(jnp.int32, (rows, rows), 1)
        counts = jnp.dot(
            mine.astype(jnp.bfloat16), before.astype(jnp.float32).astype(jnp.bfloat16),
            preferred_element_type=jnp.float32,
        )
        rank = jnp.sum(mine * counts, axis=0, keepdims=True).astype(jnp.int32)
        slot = own * (2 * CAP) + rank - 1
        for owner in range(groups):
            lane = lax.broadcasted_iota(jnp.int32, (2 * CAP, rows), 0) + owner * 2 * CAP
            for part in range(2):
                select[pl.ds(owner * 2 * CAP, 2 * CAP), pl.ds(part * rows, rows)] = (
                    (lane == slot + part * CAP).astype(jnp.float32).astype(jnp.bfloat16)
                )

    def source_terms():
        amplitude = lax.dot_general(
            res_ref[...], hist[...], contract_last, preferred_element_type=jnp.float32
        )
        mech = mech_ref[...].astype(jnp.float32)
        spare = jnp.zeros((comps - mech.shape[0], rows), jnp.float32)
        offsets = off_ref[...]
        places = [offsets // (cy * cz), (offsets // cz) % cy, offsets % cz]
        places = [p.astype(jnp.float32) for p in places]
        parts = places + [jnp.zeros((comps - 3, rows), jnp.float32)]
        for t in range(steps):
            parts += [mech * amplitude[t : t + 1, :], spare]
        parts += [jnp.zeros((2 * tall - comps * (steps + 1), rows), jnp.float32)] if 2 * tall > comps * (steps + 1) else []
        packed = jnp.concatenate(parts, axis=0)
        packed = jnp.concatenate([packed[:tall], packed[tall:]], axis=1).astype(jnp.bfloat16)
        chosen = lax.dot_general(
            packed, select[...], contract_last, preferred_element_type=jnp.float32
        ).astype(jnp.bfloat16)
        for owner in range(groups):
            src[owner] = chosen[:, owner * 2 * CAP : (owner + 1) * 2 * CAP]
        gathered[0] = src[gy]

    def source_masks():
        first_half = lax.broadcasted_iota(jnp.int32, (tall, 2 * CAP), 1) < CAP
        for pair in range(groups // 2):
            low, high = (gathered[2 * pair + i].astype(jnp.float32) for i in range(2))
            lanes = pl.ds(pair * 2 * CAP, 2 * CAP)
            values[pl.ds(0, tall), lanes] = jnp.where(first_half, low, pltpu.roll(high, CAP, 1))
            values[pl.ds(tall, tall), lanes] = jnp.where(first_half, pltpu.roll(low, CAP, 1), high)
        info = values[pl.ds(0, comps), :]
        count = info.shape[1]
        cell_plane = info[0:1] * float(cy) + info[1:2]
        plane = lax.broadcasted_iota(jnp.int32, (cx * cy, count), 0)
        plane_hot[...] = jnp.where(plane == cell_plane.astype(jnp.int32), 1.0, 0.0).astype(jnp.bfloat16)
        height = lax.broadcasted_iota(jnp.int32, (cz, count), 0)
        level_hot[...] = jnp.where(height == info[2:3].astype(jnp.int32), 1.0, 0.0).astype(jnp.bfloat16)

    def insert_sources(t):
        terms = values[pl.ds((t + 1) * comps, comps), :]
        for comp in range(0, 6, 2):
            spread = jnp.concatenate(
                [
                    level_hot[...] * terms[c : c + 1, :].astype(jnp.bfloat16)
                    for c in (comp, comp + 1)
                ],
                axis=0,
            )
            placed = lax.dot_general(
                plane_hot[...], spread, contract_last, preferred_element_type=jnp.float32
            )
            for c in range(2):
                place = S.at[comp + c, pl.ds(XP, cx), pl.ds(YP, cy), :]
                place[...] = place[...] + placed[:, c * cz : (c + 1) * cz].reshape(cx, cy, cz)

    arrivals = groups - 1
    for there, _ in list(sides[:2]) + corners:
        arrivals += there.astype(jnp.int32)

    def send_stress(t):
        def send(side):
            send_face(side, 2 * t, S, STRESS_FACES)

        at_sides(far, send)
        at_sides(near, send)
        at_corners(functools.partial(send_corner, t))
        at_sides(across, send)

    corner_stage[...] = jnp.zeros_like(corner_stage)
    pl.semaphore_wait(barrier, arrivals)
    for load in stress_loads.values():
        load.wait()
    send_stress(0)
    for load in [loads[0], loads[5], loads[6], loads[8]]:
        load.wait()
    loads[7].wait()
    source_slots()
    source_terms()
    for k in range(1, groups):
        source_copy(k).start()
    loads[1].wait()
    loads[2].wait()
    everywhere = far + near + across
    for t in range(steps):
        first, second = 2 * t, 2 * t + 1
        last = t == steps - 1
        sweep(velocity_inner)
        at_sides(everywhere, lambda side: send_face(side, second, V, VELOCITY_FACES))
        if t == 0:
            at_sides(everywhere, send_edge)
        else:
            at_sides(everywhere, lambda side: own_part(side, first))
            insert_sources(t)
        at_sides(across + near + far, lambda side: receive_face(side, first, STRESS_FACES, apply_force))
        if t == 0:
            loads[3].wait()
            loads[4].wait()
            if last:
                for k in range(1, groups):
                    source_copy(k).wait_recv()
                source_masks()
                insert_sources(0)
        sweep(functools.partial(stress_inner, last))
        if t == 0 and not last:
            for k in range(1, groups):
                source_copy(k).wait_recv()
            source_masks()
            insert_sources(0)
        if t == 0:
            at_sides(across + near + far, receive_edge, lambda side: own_part(side, first))
        at_corners(functools.partial(receive_corner, t))
        strain = functools.partial(apply_strain, s_out if last else S)
        at_sides(
            across + near + far,
            lambda side: receive_face(side, second, VELOCITY_FACES, strain, partial_velocity),
        )
        if not last:
            send_stress(t + 1)
    for t in range(steps):
        finish_faces(2 * t, STRESS_FACES)
        finish_faces(2 * t + 1, VELOCITY_FACES)
        at_corners(lambda corner: corner_copy(t, corner).wait_send())
    at_sides(everywhere, lambda side: edge_copy(side).wait_send())
    for k in range(1, groups):
        source_copy(k).wait_send()


def store_kernel(v_ref, s_ref, v_out, s_out, sem):
    copies = [pltpu.make_async_copy(v_ref, v_out, sem.at[0])]
    half = s_ref.shape[0] // 2
    for part in range(2):
        layers = pl.ds(part * half, half)
        copies.append(pltpu.make_async_copy(s_ref.at[layers], s_out.at[layers], sem.at[1 + part]))
    for copy in copies:
        copy.start()
    for copy in copies:
        copy.wait()


def local(
    velocity, stresses, buoyancy, lame_first, rigidity,
    histories, mechanism, resample, owners, cell_offsets,
):
    groups = lax.axis_size("gy")
    blocks = lax.axis_size("gx")
    rows, samples = histories.shape
    steps = resample.shape[1]
    _, cx, cy, cz = velocity.shape
    tall = 8 * -(-(steps + 1) // 2)
    f32, bf16 = jnp.float32, jnp.bfloat16
    hbm = pl.BlockSpec(memory_space=pl.ANY)
    vmem = pl.BlockSpec(memory_space=pltpu.VMEM)
    dma = pltpu.SemaphoreType.DMA
    phases = 2 * steps
    v_last, s_last = pl.pallas_call(
        functools.partial(kernel, groups, blocks, steps),
        out_shape=(
            pltpu.VMEM(velocity.shape, f32),
            pltpu.VMEM(stresses.shape, f32),
        ),
        in_specs=[hbm] * 10,
        out_specs=(vmem, vmem),
        scratch_shapes=[
            pltpu.VMEM((3, cx + 2 * XP, cy + 2 * YP, cz), f32),
            pltpu.VMEM((6, cx + 2 * XP, cy + 2 * YP, cz), f32),
            pltpu.VMEM((cx, cy, cz), f32),
            pltpu.VMEM((cx, cy, cz), f32),
            pltpu.VMEM((cx, cy, cz), f32),
            pltpu.VMEM((rows, samples), bf16),
            pltpu.VMEM((mechanism.shape[1], rows), bf16),
            pltpu.VMEM((steps, samples), bf16),
            pltpu.VMEM((1, rows), jnp.int32),
            pltpu.VMEM((1, rows), jnp.int32),
            pltpu.VMEM((groups * 2 * CAP, 2 * rows), bf16),
            pltpu.VMEM((groups, tall, 2 * CAP), bf16),
            pltpu.VMEM((groups, tall, 2 * CAP), bf16),
            pltpu.VMEM((2 * tall, groups * CAP), f32),
            pltpu.VMEM((cx * cy, groups * CAP), bf16),
            pltpu.VMEM((cz, groups * CAP), bf16),
            pltpu.VMEM((phases, 2, 9, cy, cz), bf16),
            pltpu.VMEM((phases, 2, 9, cy, cz), bf16),
            pltpu.VMEM((phases, 2, 9, cx, cz), bf16),
            pltpu.VMEM((phases, 2, 9, cx, cz), bf16),
            pltpu.VMEM((4, 16, cz), f32),
            pltpu.VMEM((steps, 4, 16, cz), bf16),
            pltpu.VMEM((steps, 4, 16, cz), bf16),
            pltpu.VMEM((2, 2, cy, cz), jnp.int16),
            pltpu.VMEM((2, 2, cy, cz), jnp.int16),
            pltpu.VMEM((2, 2, cx, cz), jnp.int16),
            pltpu.VMEM((2, 2, cx, cz), jnp.int16),
            pltpu.VMEM((2, 2, cy, cz), f32),
            pltpu.VMEM((2, 2, cx, cz), f32),
            pltpu.VMEM((2, 5, cy, cz), f32),
            pltpu.VMEM((2, 5, cx, cz), f32),
            dma((6,)),
            dma((9,)),
            dma((groups,)),
            dma((groups,)),
            dma((phases, 4)),
            dma((phases, 4)),
            dma((steps, 4)),
            dma((steps, 4)),
            dma((4,)),
            dma((4,)),
        ],
        compiler_params=pltpu.CompilerParams(collective_id=0, has_side_effects=True),
    )(
        velocity, stresses, buoyancy, lame_first, rigidity, histories, mechanism.T, resample.T,
        owners.reshape(1, rows), cell_offsets.reshape(1, rows),
    )
    return pl.pallas_call(
        store_kernel,
        out_shape=(
            jax.ShapeDtypeStruct(velocity.shape, f32),
            jax.ShapeDtypeStruct(stresses.shape, f32),
        ),
        in_specs=[vmem, vmem],
        out_specs=(hbm, hbm),
        scratch_shapes=[dma((3,))],
    )(
        pltpu.with_memory_space_constraint(v_last, pltpu.VMEM),
        pltpu.with_memory_space_constraint(s_last, pltpu.VMEM),
    )


def solution(mesh):
    in_specs = (
        P(None, "gx", "gy", None),
        P(None, "gx", "gy", None),
        P("gx", "gy", None),
        P("gx", "gy", None),
        P("gx", "gy", None),
        P(("gx", "gy"), None),
        P(("gx", "gy"), None),
        P(),
        P(("gx", "gy"), None),
        P(("gx", "gy")),
    )
    out_specs = (P(None, "gx", "gy", None), P(None, "gx", "gy", None))
    return jax.shard_map(local, mesh=mesh, in_specs=in_specs, out_specs=out_specs, check_vma=False)
```
